256 devices in a mesh: batch: 32 (over y, z_lo, core), heads: 8 (over x, z_hi).
Axes of the slice: x: 4, y: 4, z: 8 (z_hi: 2, z_lo: 4; z = z_hi * 4 + z_lo), core: 2. Of those that a mesh axis runs over, the one named last changes fastest.
Arguments:
- token_ids: int32 [256, 2, 5], P('batch'), may hold values from 0 to 65535
- accepted: int32 [256], P('batch'), may hold values from 0 to 4
- lengths: int32 [256], P('batch'), may hold values from 128 to 512
- queries: bfloat16 [256, 2, 5, 4096], P('batch', None, None, 'heads'), may hold values from -8 to 8
- new_kv: bfloat16 [256, 2, 2, 5, 1024], P('batch', None, None, None, 'heads'), may hold values from -4 to 4
- cache_kv: bfloat16 [256, 2, 512, 1024], P('batch', None, None, 'heads'), may hold values from -8 to 8
- table: bfloat16 [65536, 8192], P('heads', 'batch'), may hold values from -6 to 6
- w_out: bfloat16 [4096, 8192], P('heads', 'batch'), may hold values from -0.1875 to 0.1875
- gain: float32 [8192], P('batch'), may hold values from 0.25 to 1.75
- w_feat: bfloat16 [8192, 8192], P('batch', 'heads'), may hold values from -0.0625 to 0.0625
- w_emb: bfloat16 [8192, 8192], P('batch', 'heads'), may hold values from -0.0625 to 0.0625
Outputs:
- verified_hidden: bfloat16 [2560, 8192], P(None, 'batch')
- draft_feat: bfloat16 [256, 2, 5, 8192], P('batch', None, None, 'heads')
The draws below stay inside these ranges and needn't reach their ends.
All inputs are finite; a program needn't handle non-finite values.
Results may differ from the reference program's by a relative error of at most 0.0043.
Values may be sent and summed in bfloat16 or wider, within the bound.
No kernel may reach another device: no remote copies, remote signals or barrier semaphores. Data moves between devices by JAX's collectives and lax.ppermute only.
A program may use at most 64 MiB of HBM per device.

```python
import jax
import jax.numpy as jnp
from jax import lax

D = 8192
HQ = 32
KV = 8
HD = 128
VOCAB = 65536
DRAFT = 4
CTX = 512
ROWS = 256


def draw_cache_kv(key, part):
    noise = jnp.clip(0.5 * jax.random.normal(jax.random.fold_in(key, 2), (ROWS, 2, CTX, KV * HD), jnp.float32), -4.0, 4.0)
    return noise.astype(jnp.bfloat16)


def draw_queries(key, part):
    noise = jnp.clip(0.5 * jax.random.normal(jax.random.fold_in(key, 1), (ROWS, 2, DRAFT + 1, HQ * HD), jnp.float32), -4.0, 4.0)
    return noise.astype(jnp.bfloat16)


def with_ends(values, rng, least, top_value):
    index_at = [jax.random.randint(jax.random.fold_in(rng, axis), (), 0, length) for axis, length in enumerate(values.shape)]
    widest = values.shape.index(max(values.shape))
    next_to = index_at[:widest] + [(index_at[widest] + 1) % values.shape[widest]] + index_at[widest + 1:]
    return values.at[tuple(index_at)].set(least).at[tuple(next_to)].set(top_value)


def steps_of(key, shape, cuts, least, high):
    def one(position, shards_of):
        steps = jax.random.uniform(jax.random.fold_in(jax.random.fold_in(key, 6), position), (shards_of,), jnp.float32, least / len(cuts), high / len(cuts))
        return jnp.repeat(jnp.exp(steps), shape[position] // shards_of).reshape((-1,) + (1,) * (len(shape) - position - 1))

    level = one(*cuts[0])
    for cut in cuts[1:]:
        level = level * one(*cut)
    return level


def gaussian(own_key, shape, spread, limit, pieces=(), kind=jnp.bfloat16):
    loudness = steps_of(own_key, shape, pieces, -0.22, 0.18) if pieces else 1.0
    values = jax.random.normal(own_key, shape, jnp.float32) * spread * loudness
    return jnp.minimum(jnp.maximum(values, -limit), limit).astype(kind)


def setup_inputs(seed: int = 0) -> dict:
    streams_of = jax.random.split(jax.random.key(seed), 12)
    token_ids = with_ends(jax.random.randint(streams_of[0], (ROWS, 2, DRAFT + 1), 0, VOCAB), jax.random.fold_in(streams_of[0], 1), 0, VOCAB - 1).astype(jnp.int32)
    accepted = with_ends(jax.random.randint(streams_of[1], (ROWS,), 0, DRAFT + 1), jax.random.fold_in(streams_of[1], 1), 0, DRAFT).astype(jnp.int32)
    lengths = with_ends(jax.random.randint(streams_of[2], (ROWS,), CTX // 4, CTX + 1), jax.random.fold_in(streams_of[2], 1), CTX // 4, CTX).astype(jnp.int32)
    queries = draw_queries(jax.random.fold_in(streams_of[11], 71), 0)
    new_kv = gaussian(streams_of[4], (ROWS, 2, 2, DRAFT + 1, KV * HD), 0.5, 4.0, ((0, 32), (4, 8)))
    cache_kv = draw_cache_kv(jax.random.fold_in(streams_of[11], 71), 0)
    table = gaussian(streams_of[6], (VOCAB, D), 1.0, 6.0, ((0, 8), (1, 32)))
    w_out = gaussian(streams_of[7], (HQ * HD, D), (HQ * HD // 4) ** -0.5, 0.1875, ((0, 8), (1, 32)))
    gain = jnp.clip(1.0 + 0.15 * jax.random.normal(streams_of[8], (D,), jnp.float32), 0.25, 1.75)
    w_feat = gaussian(streams_of[9], (D, D), D ** -0.5, 0.0625, ((0, 32), (1, 8)))
    w_emb = gaussian(streams_of[10], (D, D), D ** -0.5, 0.0625, ((0, 32), (1, 8)))
    return {"token_ids": token_ids, "accepted": accepted, "lengths": lengths, "queries": queries, "new_kv": new_kv, "cache_kv": cache_kv, "table": table, "w_out": w_out, "gain": gain, "w_feat": w_feat, "w_emb": w_emb}


def attend(queries, new_kv, cache_kv, lengths, accepted):
    steps = queries.shape[2]
    group = HQ // KV
    qv = queries.reshape(ROWS, 2, steps, KV, group, HD).astype(jnp.float32)
    keys = jnp.concatenate([cache_kv[:, 0].reshape(ROWS, CTX, KV, HD), new_kv[:, :, 0].reshape(ROWS, 2 * steps, KV, HD)], axis=1)
    vals = jnp.concatenate([cache_kv[:, 1].reshape(ROWS, CTX, KV, HD), new_kv[:, :, 1].reshape(ROWS, 2 * steps, KV, HD)], axis=1)
    scores = jnp.einsum('rtigjd,rkgd->rtigjk', qv, keys.astype(jnp.float32)) / jnp.sqrt(jnp.float32(HD))
    width = CTX + 2 * steps
    slot = jnp.arange(width, dtype=jnp.int32)[None, None, None, :]
    rnd = jnp.arange(2, dtype=jnp.int32)[None, :, None, None]
    pos = jnp.arange(steps, dtype=jnp.int32)[None, None, :, None]
    first = slot - CTX
    second = slot - CTX - steps
    seen = slot < lengths[:, None, None, None]
    seen = seen | (first >= 0) & (first < steps) & ((rnd == 0) & (first <= pos) | (rnd == 1) & (first <= accepted[:, None, None, None]))
    seen = seen | (second >= 0) & (rnd == 1) & (second <= pos)
    seen = seen[:, :, :, None, None, :]
    masked = jnp.where(seen, scores, jnp.float32(-1e+30))
    top = lax.optimization_barrier(jnp.max(masked, axis=-1, keepdims=True))
    expo = jnp.where(seen, jnp.exp(masked - top), jnp.float32(0.0))
    weights = (expo / lax.optimization_barrier(jnp.sum(expo, axis=-1, keepdims=True))).astype(jnp.bfloat16)
    out = jnp.einsum('rtigjk,rkgd->rtigjd', weights.astype(jnp.float32), vals.astype(jnp.float32))
    return out.astype(jnp.bfloat16).reshape(ROWS * 2 * steps, HQ * HD)

def reference(token_ids, accepted, lengths, queries, new_kv, cache_kv, table, w_out, gain, w_feat, w_emb):
    emb_bf = jnp.take(table, token_ids.reshape(-1), axis=0)
    emb = emb_bf.astype(jnp.float32)
    attn = attend(queries, new_kv, cache_kv, lengths, accepted)
    hidden = emb + jnp.dot(attn, w_out, preferred_element_type=jnp.float32)
    scale = jax.lax.rsqrt(lax.optimization_barrier(jnp.mean(hidden * hidden, axis=1, keepdims=True)) + 1e-05)
    feat = (hidden * scale * gain[None, :]).astype(jnp.bfloat16)
    draft = jnp.dot(feat, w_feat, preferred_element_type=jnp.float32) + jnp.dot(emb_bf, w_emb, preferred_element_type=jnp.float32)
    return (hidden.astype(jnp.bfloat16), draft.astype(jnp.bfloat16).reshape(ROWS, 2, queries.shape[2], D))
```

```python
import jax
import jax.numpy as jnp
from jax import lax
from jax.experimental import pallas as pl
from jax.experimental.pallas import tpu as pltpu
from jax.sharding import PartitionSpec as P

D = 8192
HD = 128
Y, Z, C, X, W = 4, 4, 2, 4, 2
BF = jnp.bfloat16
F32 = jnp.float32


def route(array, move):
    pairs = []
    for y in range(Y):
        for z in range(Z):
            for c in range(C):
                for x in range(X):
                    for w in range(W):
                        ty, tz, tc, tx, tw = move(y, z, c, x, w)
                        ty, tz, tc, tx, tw = ty % Y, tz % Z, tc % C, tx % X, tw % W
                        source = ((y * Z + z) * C + c) * X * W + x * W + w
                        target = ((ty * Z + tz) * C + tc) * X * W + tx * W + tw
                        pairs.append((source, target))
    return lax.ppermute(array, ("batch", "heads"), pairs)


def over_core(array):
    return route(array, lambda y, z, c, x, w: (y, z, c + 1, x, w))


def over_half(array):
    return route(array, lambda y, z, c, x, w: (y, z, c, x, w + 1))


def along_x(array, k):
    return route(array, lambda y, z, c, x, w: (y, z, c, x + k, w))


def from_everyone(array, axis):
    devices = lax.axis_size(axis)
    return lax.all_to_all(
        jnp.broadcast_to(array[None], (devices, *array.shape)), axis, 0, 0, tiled=True
    )


def turned(array, axis, start):
    n = array.shape[axis]
    back = jnp.flip(array, axis)
    twice = jnp.concatenate([back, back], axis=axis)
    return lax.dynamic_slice_in_dim(twice, (n - 1 - start) % n, n, axis)


def risen(array, axis, start):
    n = array.shape[axis]
    twice = jnp.concatenate([array, array], axis=axis)
    return lax.dynamic_slice_in_dim(twice, start % n, n, axis)


def attend_local(queries, new_kv, cache_kv, lengths, accepted):
    rows, _, steps, qcols = queries.shape
    slots = cache_kv.shape[2]
    kv_heads = cache_kv.shape[3] // HD
    q_heads = qcols // HD
    group = q_heads // kv_heads
    qv = queries.reshape(rows, 2, steps, kv_heads, group, HD)
    keys = jnp.concatenate(
        [
            cache_kv[:, 0].reshape(rows, slots, kv_heads, HD),
            new_kv[:, :, 0].reshape(rows, 2 * steps, kv_heads, HD),
        ],
        axis=1,
    )
    vals = jnp.concatenate(
        [
            cache_kv[:, 1].reshape(rows, slots, kv_heads, HD),
            new_kv[:, :, 1].reshape(rows, 2 * steps, kv_heads, HD),
        ],
        axis=1,
    )
    scores = jnp.einsum(
        "rtigjd,rkgd->rtigjk", qv, keys, preferred_element_type=F32
    ) / jnp.sqrt(jnp.float32(HD))
    width = slots + 2 * steps
    slot = jnp.arange(width, dtype=jnp.int32)[None, None, None, :]
    rnd = jnp.arange(2, dtype=jnp.int32)[None, :, None, None]
    pos = jnp.arange(steps, dtype=jnp.int32)[None, None, :, None]
    first = slot - slots
    second = slot - slots - steps
    seen = slot < lengths[:, None, None, None]
    seen = seen | (first >= 0) & (first < steps) & (
        (rnd == 0) & (first <= pos) | (rnd == 1) & (first <= accepted[:, None, None, None])
    )
    seen = seen | (second >= 0) & (rnd == 1) & (second <= pos)
    seen = seen[:, :, :, None, None, :]
    masked = jnp.where(seen, scores, jnp.float32(-1e30))
    top = jnp.max(masked, axis=-1, keepdims=True)
    expo = jnp.where(seen, jnp.exp(masked - top), jnp.float32(0.0))
    weights = (expo / jnp.sum(expo, axis=-1, keepdims=True)).astype(BF)
    out = jnp.einsum("rtigjk,rkgd->rtigjd", weights, vals, preferred_element_type=F32)
    return out.astype(BF).reshape(rows * 2 * steps, qcols)


def placed_kernel(at_ref, own_ref, other_ref, out_ref):
    side = pl.program_id(1)

    @pl.when(side == 0)
    def _():
        out_ref[...] = own_ref[...][None]

    @pl.when(side == 1)
    def _():
        out_ref[...] = other_ref[...][None]


def placed(own, other, block_of, core):
    blocks, n, cols = own.shape
    at = jnp.concatenate([block_of.reshape(-1), core.reshape(1)]).astype(jnp.int32)
    return pl.pallas_call(
        placed_kernel,
        grid_spec=pltpu.PrefetchScalarGridSpec(
            num_scalar_prefetch=1,
            grid=(blocks, 2),
            in_specs=[
                pl.BlockSpec((1, n, cols), lambda i, s, at: (i, 0, 0)),
                pl.BlockSpec((1, n, cols), lambda i, s, at: (i, 0, 0)),
            ],
            out_specs=pl.BlockSpec(
                (1, 1, n, cols), lambda i, s, at: (at[i], (at[blocks] + s) % 2, 0, 0)
            ),
        ),
        out_shape=jax.ShapeDtypeStruct((blocks, 2, n, cols), own.dtype),
        name="placed",
    )(at, own, other)


def body(
    token_ids, accepted, lengths, queries, new_kv, cache_kv, table, w_out, gain, w_feat, w_emb
):
    rows, _, steps = token_ids.shape
    n = rows * 2 * steps
    b, h = lax.axis_index("batch"), lax.axis_index("heads")
    y, z, c = b // (Z * C), b // C % Z, b % C
    x, w = h // W, h % W

    w_out2 = jnp.concatenate([w_out, over_core(w_out)], axis=1)
    w_feat2 = jnp.concatenate([w_feat, over_core(w_feat)], axis=0)
    w_emb2 = jnp.concatenate([w_emb, over_core(w_emb)], axis=0)
    gain2 = jnp.concatenate([gain, over_core(gain)])
    cols = w_out2.shape[1]

    ids = from_everyone(token_ids.reshape(-1), "batch").reshape(Y, Z, C, n)
    ids = turned(turned(ids, 0, (y - x) % Y), 1, (z - 2 * w) % Z)
    ids = risen(jnp.moveaxis(ids, 2, 0), 0, c).reshape(-1)
    vocab_rows = table.shape[0]
    local_ids = ids - h * vocab_rows
    inside = (local_ids >= 0) & (local_ids < vocab_rows)
    picked = jnp.take(table, jnp.clip(local_ids, 0, vocab_rows - 1), axis=0)
    picked = jnp.where(inside[:, None], picked, jnp.zeros((), BF))
    half = picked.shape[0] // 2
    part_emb = jnp.concatenate([picked[:half], over_core(picked[half:])], axis=1)
    part_emb = part_emb.reshape(Y, Z * n, cols)
    emb_sum = part_emb[0]
    for k in range(1, X):
        emb_sum = emb_sum + along_x(part_emb[k], k)
    emb_share = emb_sum[: 2 * n] + over_half(emb_sum[2 * n :])
    emb_block = jnp.concatenate([emb_share, over_half(emb_share)], axis=0)
    emb = [emb_block] + [along_x(emb_block, k) for k in range(1, X)]

    attn = attend_local(queries, new_kv, cache_kv, lengths, accepted)
    attn = jnp.concatenate(
        [
            route(attn, lambda y, z, c, x, w: (y, z + k + 2 * w, c, x, w))
            for k in range(Z)
        ],
        axis=0,
    )
    attn = [route(attn, lambda y, z, c, x, w: (y + k + x, z, c, x, w)) for k in range(Y)]
    part = [jnp.dot(a, w_out2, preferred_element_type=F32) for a in attn]
    proj_sum = part[0]
    for k in range(1, X):
        proj_sum = proj_sum + along_x(part[k].astype(BF), k).astype(F32)
    proj_share = proj_sum[: 2 * n] + over_half(proj_sum[2 * n :].astype(BF)).astype(F32)
    proj_share = proj_share.astype(BF)
    proj_block = jnp.concatenate([proj_share, over_half(proj_share)], axis=0)
    proj = [proj_block] + [along_x(proj_block, k) for k in range(1, X)]

    hidden_share = emb_share.astype(F32) + proj_share.astype(F32)
    squares = jnp.sum(hidden_share * hidden_share, axis=1)
    squares = from_everyone(squares, "heads").reshape(Y, Z, n)
    squares = turned(turned(squares, 0, y), 1, z)
    squares = from_everyone(squares.reshape(-1), "batch").reshape(Y * Z, C, Y, Z, n)
    squares = jnp.sum(squares, axis=0)
    squares = lax.dynamic_index_in_dim(squares, c, 0, keepdims=False)
    squares = turned(risen(squares, 0, (y - x) % Y), 1, (z - 2 * w) % Z)
    scale = lax.rsqrt(squares / D + 1e-05).reshape(Y, Z * n, 1)

    summed, own, other = None, [], []
    for k in range(X):
        hidden = emb[k].astype(F32) + proj[k].astype(F32)
        verified = hidden.astype(BF)
        own.append(verified[:, : cols // 2])
        other.append(verified[:, cols // 2 :])
        feat = (hidden * scale[k] * gain2[None, :]).astype(BF)
        draft = jnp.dot(feat, w_feat2, preferred_element_type=F32) + jnp.dot(
            emb[k], w_emb2, preferred_element_type=F32
        )
        got = route(draft.astype(BF), lambda y, z, c, x, w: (y + k - x, z, c, x, w)).astype(F32)
        summed = got if summed is None else summed + got
    total = None
    for k in range(Z):
        got = route(
            summed[k * n : (k + 1) * n].astype(BF),
            lambda y, z, c, x, w: (y, z - k - 2 * w, c, x, w),
        ).astype(F32)
        total = got if total is None else total + got
    draft = total.astype(BF).reshape(rows, 2, steps, w_feat.shape[1])

    own = jnp.concatenate(own, axis=0).reshape(Y * Z, n, cols // 2)
    other = over_core(jnp.concatenate(other, axis=0)).reshape(Y * Z, n, cols // 2)
    step = jnp.arange(4, dtype=jnp.int32)
    block_of = ((y - x + step) % Y)[:, None] * Z + ((z - 2 * w - step) % Z)[None, :]
    verified = placed(own, other, block_of, c).reshape(Y * Z * C * n, cols // 2)
    return (verified, draft)


def solution(mesh):
    placed_in = (
        P("batch", None, None),
        P("batch"),
        P("batch"),
        P("batch", None, None, "heads"),
        P("batch", None, None, None, "heads"),
        P("batch", None, None, "heads"),
        P("heads", "batch"),
        P("heads", "batch"),
        P("batch"),
        P("batch", "heads"),
        P("batch", "heads"),
    )
    return jax.shard_map(
        body,
        mesh=mesh,
        in_specs=placed_in,
        out_specs=(P(None, "batch"), P("batch", None, None, "heads")),
        check_vma=False,
    )
```

```python
import jax
import jax.numpy as jnp
from jax import lax
from jax.experimental import pallas as pl
from jax.experimental.pallas import tpu as pltpu
from jax.sharding import PartitionSpec as P

D = 8192
HD = 128
Y, Z, C, X, W = 4, 4, 2, 4, 2
BF = jnp.bfloat16
F32 = jnp.float32


def route(array, move):
    pairs = []
    for y in range(Y):
        for z in range(Z):
            for c in range(C):
                for x in range(X):
                    for w in range(W):
                        ty, tz, tc, tx, tw = move(y, z, c, x, w)
                        ty, tz, tc, tx, tw = ty % Y, tz % Z, tc % C, tx % X, tw % W
                        source = ((y * Z + z) * C + c) * X * W + x * W + w
                        target = ((ty * Z + tz) * C + tc) * X * W + tx * W + tw
                        pairs.append((source, target))
    return lax.ppermute(array, ("batch", "heads"), pairs)


def over_core(array):
    return route(array, lambda y, z, c, x, w: (y, z, c + 1, x, w))


def over_half(array):
    return route(array, lambda y, z, c, x, w: (y, z, c, x, w + 1))


def along_x(array, k):
    return route(array, lambda y, z, c, x, w: (y, z, c, x + k, w))


def from_everyone(array, axis):
    devices = lax.axis_size(axis)
    return lax.all_to_all(
        jnp.broadcast_to(array[None], (devices, *array.shape)), axis, 0, 0, tiled=True
    )


def risen(array, axis, start):
    n = array.shape[axis]
    twice = jnp.concatenate([array, array], axis=axis)
    return lax.dynamic_slice_in_dim(twice, start % n, n, axis)


def attend_local(queries, new_kv, cache_kv, lengths, accepted):
    rows, _, steps, qcols = queries.shape
    slots = cache_kv.shape[2]
    kv_heads = cache_kv.shape[3] // HD
    q_heads = qcols // HD
    group = q_heads // kv_heads
    qv = queries.reshape(rows, 2, steps, kv_heads, group, HD)
    keys = jnp.concatenate(
        [
            cache_kv[:, 0].reshape(rows, slots, kv_heads, HD),
            new_kv[:, :, 0].reshape(rows, 2 * steps, kv_heads, HD),
        ],
        axis=1,
    )
    vals = jnp.concatenate(
        [
            cache_kv[:, 1].reshape(rows, slots, kv_heads, HD),
            new_kv[:, :, 1].reshape(rows, 2 * steps, kv_heads, HD),
        ],
        axis=1,
    )
    scores = jnp.einsum(
        "rtigjd,rkgd->rtigjk", qv, keys, preferred_element_type=F32
    ) / jnp.sqrt(jnp.float32(HD))
    width = slots + 2 * steps
    slot = jnp.arange(width, dtype=jnp.int32)[None, None, None, :]
    rnd = jnp.arange(2, dtype=jnp.int32)[None, :, None, None]
    pos = jnp.arange(steps, dtype=jnp.int32)[None, None, :, None]
    first = slot - slots
    second = slot - slots - steps
    seen = slot < lengths[:, None, None, None]
    seen = seen | (first >= 0) & (first < steps) & (
        (rnd == 0) & (first <= pos) | (rnd == 1) & (first <= accepted[:, None, None, None])
    )
    seen = seen | (second >= 0) & (rnd == 1) & (second <= pos)
    seen = seen[:, :, :, None, None, :]
    masked = jnp.where(seen, scores, jnp.float32(-1e30))
    top = jnp.max(masked, axis=-1, keepdims=True)
    expo = jnp.where(seen, jnp.exp(masked - top), jnp.float32(0.0))
    weights = (expo / jnp.sum(expo, axis=-1, keepdims=True)).astype(BF)
    out = jnp.einsum("rtigjk,rkgd->rtigjd", weights, vals, preferred_element_type=F32)
    return out.astype(BF).reshape(rows * 2 * steps, qcols)


def placed_kernel(own_ref, other_ref, out_ref, sems):
    b, h = lax.axis_index("batch"), lax.axis_index("heads")
    y, c, x = b // (Z * C), b % C, h // W
    copies = []
    for i in range(16):
        at = (y + i // 4) % 4 * 4 + (x + 4 - i % 4) % 4
        copies.append(pltpu.make_async_copy(own_ref.at[i], out_ref.at[at, c], sems.at[0, i]))
        copies.append(
            pltpu.make_async_copy(other_ref.at[i], out_ref.at[at, 1 - c], sems.at[1, i])
        )
    for copy in copies:
        copy.start()
    for copy in copies:
        copy.wait()


def placed(own, other):
    blocks, n, cols = own.shape
    anywhere = pl.BlockSpec(memory_space=pl.ANY)
    return pl.pallas_call(
        placed_kernel,
        in_specs=[anywhere, anywhere],
        out_specs=anywhere,
        scratch_shapes=[pltpu.SemaphoreType.DMA((2, 16))],
        out_shape=jax.ShapeDtypeStruct((blocks, 2, n, cols), own.dtype),
        name="placed",
    )(own, other)


def body(
    token_ids, accepted, lengths, queries, new_kv, cache_kv, table, w_out, gain, w_feat, w_emb
):
    rows, _, steps = token_ids.shape
    n = rows * 2 * steps
    b, h = lax.axis_index("batch"), lax.axis_index("heads")
    y, z, c = b // (Z * C), b // C % Z, b % C
    x = h // W
    own_cols = w_out.shape[1]

    with jax.named_scope("attend"):
        attn = attend_local(queries, new_kv, cache_kv, lengths, accepted)
    slots = []
    for k in range(4):
        with jax.named_scope(f"turn{k}"):
            slots.append(route(attn, lambda y, z, c, x, w: (y, x + k, c, z, w)))
    attn = jnp.concatenate(slots, axis=1)

    with jax.named_scope("ids"):
        ids = from_everyone(token_ids.reshape(-1), "batch").reshape(Y, Z, C, n)
    ids = risen(risen(risen(ids, 0, y), 1, x), 2, c)
    ids = jnp.swapaxes(ids, 0, 1).reshape(-1)

    blocks = [attn]
    for k in range(1, 4):
        with jax.named_scope(f"ally{k}"):
            blocks.append(route(attn, lambda y, z, c, x, w: (y + k, z, c, x, w)))
    attn = jnp.concatenate(blocks, axis=0)

    outs = [w_out]
    for k in range(1, 4):
        with jax.named_scope(f"wout{k}"):
            outs.append(route(w_out, lambda y, z, c, x, w: (y, z, c, x + k, w)))
    outs = risen(jnp.stack(outs), 0, (x - z) % 4).reshape(-1, own_cols)
    w_all = jnp.concatenate([outs, over_core(outs)], axis=1)

    high = gain.astype(BF)
    mid = (gain - high.astype(F32)).astype(BF)
    low = (gain - high.astype(F32) - mid.astype(F32)).astype(BF)
    extra = jnp.concatenate([high, mid, low, jnp.zeros_like(low)]).reshape(1, -1)
    extra = jnp.pad(extra, ((0, 15), (0, w_feat.shape[1] - extra.shape[1])))
    pack = [jnp.concatenate([w_feat, w_emb, extra], axis=0)]
    for k in range(1, 4):
        with jax.named_scope(f"wdraft{k}"):
            pack.append(route(pack[0], lambda y, z, c, x, w: (y + k, z, c, x, w)))
    pack = pack + [over_core(p) for p in pack]
    w_feats = jnp.concatenate([p[:own_cols] for p in pack], axis=0)
    w_embs = jnp.concatenate([p[own_cols : 2 * own_cols] for p in pack], axis=0)
    gains = jnp.stack([p[2 * own_cols, : 3 * own_cols] for p in pack]).astype(F32)
    gains = gains.reshape(8, 3, own_cols)
    gains = ((gains[:, 0] + gains[:, 1]) + gains[:, 2]).reshape(1, -1)

    vocab_rows = table.shape[0]
    local_ids = ids - h * vocab_rows
    inside = (local_ids >= 0) & (local_ids < vocab_rows)
    with jax.named_scope("pick"):
        picked = jnp.take(table, jnp.clip(local_ids, 0, vocab_rows - 1), axis=0)
        picked = jnp.where(inside[:, None], picked, jnp.zeros((), BF))
    picked = picked.reshape(4, 4 * 2 * n, own_cols)
    emb = picked[0]
    for k in range(1, 4):
        with jax.named_scope(f"embx{k}"):
            emb = emb + along_x(picked[k], k)
    emb = emb.reshape(4, 2, n, own_cols)
    pieces = [emb[0]]
    for k in range(1, 4):
        with jax.named_scope(f"emby{k}"):
            pieces.append(route(emb[k], lambda y, z, c, x, w: (y + k, z, c, x, w)))
    kept = jnp.concatenate([p[0] for p in pieces], axis=1)
    with jax.named_scope("embc"):
        got = over_core(jnp.concatenate([p[1] for p in pieces], axis=1))
    emb = jnp.concatenate([kept, got], axis=1)
    with jax.named_scope("embz"):
        emb = emb + over_half(emb)
    embs = [emb]
    for k in range(1, 4):
        with jax.named_scope(f"emba{k}"):
            embs.append(along_x(emb, k))

    part = jnp.dot(attn, w_all, preferred_element_type=F32).astype(BF).reshape(4, n, -1)
    pieces = [part[0]]
    for k in range(1, 4):
        with jax.named_scope(f"projy{k}"):
            pieces.append(route(part[4 - k], lambda y, z, c, x, w: (y + k, z, c, x, w)))
    proj = jnp.concatenate(
        [p[:, :own_cols] for p in pieces] + [p[:, own_cols:] for p in pieces], axis=1
    )
    with jax.named_scope("projz"):
        proj = (proj.astype(F32) + over_half(proj).astype(F32)).astype(BF)
    projs = [proj]
    for k in range(1, 4):
        with jax.named_scope(f"proja{k}"):
            projs.append(along_x(proj, k))

    hidden = emb.astype(F32) + proj.astype(F32)
    squares = jnp.sum(hidden * hidden, axis=1)
    total = squares
    for k in range(1, 4):
        with jax.named_scope(f"sumz{k}"):
            total = total + route(squares, lambda y, z, c, x, w: (y, z + k, c, x, w))
    scale = lax.rsqrt(total / D + 1e-05)
    scales = [scale]
    for k in range(1, 4):
        with jax.named_scope(f"scalex{k}"):
            scales.append(along_x(scale, k))

    emb = jnp.concatenate(embs, axis=0)
    hidden = emb.astype(F32) + jnp.concatenate(projs, axis=0).astype(F32)
    feat = (hidden * jnp.concatenate(scales)[:, None] * gains).astype(BF)
    draft = jnp.dot(emb, w_embs, preferred_element_type=F32)
    draft = draft + jnp.dot(feat, w_feats, preferred_element_type=F32)
    draft = draft.astype(BF).reshape(4, n, -1)
    total = None
    for k in range(4):
        piece = lax.dynamic_index_in_dim(draft, (x - z - k) % 4, 0, keepdims=False)
        if k:
            with jax.named_scope(f"draftz{k}"):
                piece = route(piece, lambda y, z, c, x, w: (y, z + k, c, x, w))
        total = piece.astype(F32) if total is None else total + piece.astype(F32)
    draft = total.astype(BF).reshape(rows, 2, steps, w_feat.shape[1])

    verified = hidden.astype(BF)
    half = 4 * own_cols
    pieces = []
    for k in range(4):
        cut = slice(k * own_cols, (k + 1) * own_cols)
        piece = jnp.concatenate([verified[:, :half][:, cut], verified[:, half:][:, cut]], axis=1)
        if k:
            with jax.named_scope(f"very{k}"):
                piece = route(piece, lambda y, z, c, x, w: (y - k, z, c, x, w))
        pieces.append(piece)
    own = jnp.concatenate([p[:, :own_cols] for p in pieces], axis=0)
    with jax.named_scope("verc"):
        other = over_core(jnp.concatenate([p[:, own_cols:] for p in pieces], axis=0))
    verified = placed(own.reshape(16, n, own_cols), other.reshape(16, n, own_cols))
    return (verified.reshape(-1, own_cols), draft)


def solution(mesh):
    placed_in = (
        P("batch", None, None),
        P("batch"),
        P("batch"),
        P("batch", None, None, "heads"),
        P("batch", None, None, None, "heads"),
        P("batch", None, None, "heads"),
        P("heads", "batch"),
        P("heads", "batch"),
        P("batch"),
        P("batch", "heads"),
        P("batch", "heads"),
    )
    return jax.shard_map(
        body,
        mesh=mesh,
        in_specs=placed_in,
        out_specs=(P(None, "batch"), P("batch", None, None, "heads")),
        check_vma=False,
    )
```

```python
import jax
import jax.numpy as jnp
from jax import lax
from jax.experimental import pallas as pl
from jax.experimental.pallas import tpu as pltpu
from jax.sharding import PartitionSpec as P


D = 8192
HD = 128
Y, Z, C, X, W = 4, 4, 2, 4, 2
BF = jnp.bfloat16
F32 = jnp.float32


def route(array, move):
    pairs = []
    for y in range(Y):
        for z in range(Z):
            for c in range(C):
                for x in range(X):
                    for w in range(W):
                        ty, tz, tc, tx, tw = move(y, z, c, x, w)
                        ty, tz, tc, tx, tw = ty % Y, tz % Z, tc % C, tx % X, tw % W
                        source = ((y * Z + z) * C + c) * X * W + x * W + w
                        target = ((ty * Z + tz) * C + tc) * X * W + tx * W + tw
                        pairs.append((source, target))
    return lax.ppermute(array, ("batch", "heads"), pairs)


def over_core(array):
    return route(array, lambda y, z, c, x, w: (y, z, c + 1, x, w))


def over_half(array):
    return route(array, lambda y, z, c, x, w: (y, z, c, x, w + 1))


def along_x(array, k):
    return route(array, lambda y, z, c, x, w: (y, z, c, x + k, w))


def from_everyone(array, axis):
    devices = lax.axis_size(axis)
    return lax.all_to_all(
        jnp.broadcast_to(array[None], (devices, *array.shape)), axis, 0, 0, tiled=True
    )


def risen(array, axis, start):
    n = array.shape[axis]
    twice = jnp.concatenate([array, array], axis=axis)
    return lax.dynamic_slice_in_dim(twice, start % n, n, axis)


def attend_local(queries, new_kv, cache_kv, lengths, accepted):
    rows, _, steps, qcols = queries.shape
    slots = cache_kv.shape[2]
    kv_heads = cache_kv.shape[3] // HD
    q_heads = qcols // HD
    group = q_heads // kv_heads
    qv = queries.reshape(rows, 2, steps, kv_heads, group, HD)
    keys = jnp.concatenate(
        [
            cache_kv[:, 0].reshape(rows, slots, kv_heads, HD),
            new_kv[:, :, 0].reshape(rows, 2 * steps, kv_heads, HD),
        ],
        axis=1,
    )
    vals = jnp.concatenate(
        [
            cache_kv[:, 1].reshape(rows, slots, kv_heads, HD),
            new_kv[:, :, 1].reshape(rows, 2 * steps, kv_heads, HD),
        ],
        axis=1,
    )
    scores = jnp.einsum(
        "rtigjd,rkgd->rtigjk", qv, keys, preferred_element_type=F32
    ) / jnp.sqrt(jnp.float32(HD))
    width = slots + 2 * steps
    slot = jnp.arange(width, dtype=jnp.int32)[None, None, None, :]
    rnd = jnp.arange(2, dtype=jnp.int32)[None, :, None, None]
    pos = jnp.arange(steps, dtype=jnp.int32)[None, None, :, None]
    first = slot - slots
    second = slot - slots - steps
    seen = slot < lengths[:, None, None, None]
    seen = seen | (first >= 0) & (first < steps) & (
        (rnd == 0) & (first <= pos) | (rnd == 1) & (first <= accepted[:, None, None, None])
    )
    seen = seen | (second >= 0) & (rnd == 1) & (second <= pos)
    seen = seen[:, :, :, None, None, :]
    masked = jnp.where(seen, scores, jnp.float32(-1e30))
    top = jnp.max(masked, axis=-1, keepdims=True)
    expo = jnp.where(seen, jnp.exp(masked - top), jnp.float32(0.0))
    weights = (expo / jnp.sum(expo, axis=-1, keepdims=True)).astype(BF)
    out = jnp.einsum("rtigjk,rkgd->rtigjd", weights, vals, preferred_element_type=F32)
    return out.astype(BF).reshape(rows * 2 * steps, qcols)


def position():
    b, h = lax.axis_index("batch"), lax.axis_index("heads")
    return b // (Z * C), b // C % Z, b % C, h // W


def project_kernel(*refs):
    lines, own, other, outs = refs[:4], refs[4:8], refs[8:12], refs[12:16]
    attn, weights, sems = refs[16:]
    _, z, _, x = position()
    rows, cols = lines[0].shape[0], own[0].shape[1]
    copies = []
    for k in range(4):
        at = (k + z - x + 4) % 4
        copies.append(
            pltpu.make_async_copy(own[k], weights.at[at, :, pl.ds(0, cols)], sems.at[0, k])
        )
        copies.append(
            pltpu.make_async_copy(other[k], weights.at[at, :, pl.ds(cols, cols)], sems.at[1, k])
        )
        copies.append(
            pltpu.make_async_copy(lines[k], attn.at[pl.ds(k * rows, rows)], sems.at[2, k])
        )
    for copy in copies:
        copy.start()
    for copy in copies:
        copy.wait()
    depth = own[0].shape[0]
    total = None
    for k in range(4):
        part = jnp.dot(
            attn[:, k * depth : (k + 1) * depth], weights[k], preferred_element_type=F32
        )
        total = part if total is None else total + part
    total = total.astype(BF)
    for k in range(4):
        outs[k][...] = total[k * rows : (k + 1) * rows]


def project(lines, own, other):
    rows, (depth, cols) = lines[0].shape[0], own[0].shape
    anywhere = pl.BlockSpec(memory_space=pl.ANY)
    return pl.pallas_call(
        project_kernel,
        in_specs=[anywhere] * 12,
        out_shape=[jax.ShapeDtypeStruct((rows, 2 * cols), BF)] * 4,
        scratch_shapes=[
            pltpu.VMEM((4 * rows, 4 * depth), BF),
            pltpu.VMEM((4, depth, 2 * cols), BF),
            pltpu.SemaphoreType.DMA((3, 4)),
        ],
        name="project",
    )(*lines, *own, *other)


def verified_kernel(*refs):
    embs, projs, outs = refs[:4], refs[4:8], refs[9:]
    rows, width = embs[0].shape
    cols = width // 8
    for k in range(4):
        hidden = (embs[k][...].astype(F32) + projs[k][...].astype(F32)).astype(BF)
        for e in range(4):
            for s in range(2):
                outs[e][k * rows : (k + 1) * rows, s * cols : (s + 1) * cols] = hidden[
                    :, (4 * s + e) * cols : (4 * s + e + 1) * cols
                ]


def verified_pieces(embs, projs, after):
    rows, width = embs[0].shape
    return pl.pallas_call(
        verified_kernel,
        out_shape=[jax.ShapeDtypeStruct((4 * rows, width // 4), BF)] * 4,
        name="verified_pieces",
    )(*embs, *projs, after)


def based_kernel(*refs):
    embs, packs, out_ref, emb = refs[:4], refs[4:12], refs[13], refs[14]
    rows, width = embs[0].shape
    depth, tile = width // 8, 256
    for k in range(4):
        emb[k * rows : (k + 1) * rows] = embs[k][...]
    for j in range(out_ref.shape[1] // tile):
        out = slice(j * tile, (j + 1) * tile)
        total = None
        for p in range(8):
            part = jnp.dot(
                emb[:, p * depth : (p + 1) * depth],
                packs[p][depth : 2 * depth, out],
                preferred_element_type=F32,
            )
            total = part if total is None else total + part
        out_ref[:, out] = total


def based(embs, packs, after):
    rows, width = embs[0].shape
    return pl.pallas_call(
        based_kernel,
        out_shape=jax.ShapeDtypeStruct((4 * rows, packs[0].shape[1]), F32),
        scratch_shapes=[pltpu.VMEM((4 * rows, width), BF)],
        name="based",
    )(*embs, *packs, after)


def draft_kernel(*refs):
    embs, projs, scales, packs, base_ref = refs[:4], refs[4:8], refs[8:12], refs[12:20], refs[20]
    outs, feat, sums = refs[21:25], refs[25], refs[26]
    _, z, _, x = position()
    rows, width = embs[0].shape
    depth, tile = width // 8, 256
    gains = []
    for p in range(8):
        extra = packs[p][2 * depth : 2 * depth + 8, :depth].astype(F32)
        gains.append((extra[0:1] + extra[1:2]) + extra[2:3])
    for k in range(4):
        scale = scales[k][:, :1]
        for p in range(8):
            cut = slice(p * depth, (p + 1) * depth)
            hidden = embs[k][:, cut].astype(F32) + projs[k][:, cut].astype(F32)
            feat[k * rows : (k + 1) * rows, cut] = (hidden * scale * gains[p]).astype(BF)
    for j in range(outs[0].shape[1] // tile):
        out = slice(j * tile, (j + 1) * tile)
        total = base_ref[:, out]
        for p in range(8):
            total = total + jnp.dot(
                feat[:, p * depth : (p + 1) * depth],
                packs[p][:depth, out],
                preferred_element_type=F32,
            )
        sums[:, :, out] = total.astype(BF).reshape(4, rows, tile)
    for k in range(4):
        outs[k][...] = sums[(x - z - k + 8) % 4]


def drafted(embs, projs, scales, packs, base):
    rows, width = embs[0].shape
    cols = packs[0].shape[1]
    return pl.pallas_call(
        draft_kernel,
        out_shape=[jax.ShapeDtypeStruct((rows, cols), BF)] * 4,
        scratch_shapes=[
            pltpu.VMEM((4 * rows, width), BF),
            pltpu.VMEM((4, rows, cols), BF),
        ],
        name="drafted",
    )(*embs, *projs, *scales, *packs, base)


def halves_kernel(*refs):
    ins, out_ref = refs[:4], refs[-1]
    cols = out_ref.shape[2]
    for k, ref in enumerate(ins):
        out_ref[k] = ref[:, cols:]


def second_halves(pieces, after):
    rows, width = pieces[0].shape
    return pl.pallas_call(
        halves_kernel,
        out_shape=jax.ShapeDtypeStruct((4, rows, width // 2), BF),
        name="second_halves",
    )(*pieces, after)


def placed_kernel(*refs):
    pieces, other_ref, out_ref = refs[:4], refs[4], refs[5]
    y, _, c, x = position()
    rows, cols = out_ref.shape[2:]
    for e in range(4):
        for k in range(4):
            at = (y + e) % 4 * 4 + (x + 4 - k) % 4
            cut = slice(k * rows, (k + 1) * rows)
            out_ref[at, c] = pieces[e][cut, :cols]
            out_ref[at, 1 - c] = other_ref[e, cut]


def placed(pieces, other):
    rows, width = pieces[0].shape
    return pl.pallas_call(
        placed_kernel,
        out_shape=jax.ShapeDtypeStruct((16, 2, rows // 4, width // 2), BF),
        name="placed",
    )(*pieces, other)


def step(
    token_ids, accepted, lengths, queries, new_kv, cache_kv, table, w_out, gain, w_feat, w_emb
):
    rows, _, steps = token_ids.shape
    n = rows * 2 * steps
    y, _, c, x = position()
    h = lax.axis_index("heads")
    own_cols = w_out.shape[1]

    outs = [w_out]
    for k in range(1, 4):
        outs.append(route(w_out, lambda y, z, c, x, w: (y, z, c, x + k, w)))

    ids = from_everyone(token_ids.reshape(-1), "batch").reshape(Y, Z, C, n)
    ids = risen(risen(risen(ids, 0, y), 1, x), 2, c)
    ids = jnp.swapaxes(ids, 0, 1).reshape(-1)

    high = gain.astype(BF)
    mid = (gain - high.astype(F32)).astype(BF)
    low = (gain - high.astype(F32) - mid.astype(F32)).astype(BF)
    extra = jnp.stack([high, mid, low])
    extra = jnp.pad(extra, ((0, 13), (0, w_feat.shape[1] - extra.shape[1])))
    pack = [jnp.concatenate([w_feat, w_emb, extra], axis=0)]
    for k in range(1, 4):
        pack.append(route(pack[0], lambda y, z, c, x, w: (y + k, z, c, x, w)))

    attn = attend_local(queries, new_kv, cache_kv, lengths, accepted)
    slots = []
    for k in range(4):
        slots.append(route(attn, lambda y, z, c, x, w: (y, x + k, c, z, w)))
    attn = jnp.concatenate(slots, axis=1)
    lines = [attn]
    for k in range(1, 4):
        lines.append(route(attn, lambda y, z, c, x, w: (y + k, z, c, x, w)))

    vocab_rows = table.shape[0]
    local_ids = ids - h * vocab_rows
    inside = ((local_ids >= 0) & (local_ids < vocab_rows)).reshape(-1, 128)
    local_ids = jnp.clip(local_ids, 0, vocab_rows - 1)
    eye = jnp.arange(128)[:, None] == jnp.arange(128)[None, :]
    found = table.at[local_ids].get(mode="promise_in_bounds")
    keep = (eye[None] & inside[:, None, :]).astype(BF)
    found = lax.dot_general(
        keep,
        found.reshape(-1, 128, own_cols),
        (((2,), (1,)), ((0,), (0,))),
        preferred_element_type=F32,
    )
    found = found.astype(BF).reshape(4, 4 * 2 * n, own_cols)
    emb = found[0]
    for k in (2, 1, 3):
        emb = emb + along_x(found[k], k)
    emb = emb.reshape(4, 2, n, own_cols)
    pieces = [emb[0]]
    for k in range(1, 4):
        pieces.append(route(emb[k], lambda y, z, c, x, w: (y + k, z, c, x, w)))
    give = jnp.concatenate([p[1] for p in pieces], axis=1)
    got = over_core(give)
    emb = jnp.concatenate([p[0] for p in pieces] + [got], axis=1)
    emb = lax.optimization_barrier(emb + over_half(emb))
    embs = [emb]
    for k in range(1, 4):
        embs.append(along_x(emb, k))

    part = project(lines, outs, [over_core(p) for p in outs])
    pieces = [part[0]]
    for k in range(1, 4):
        pieces.append(route(part[4 - k], lambda y, z, c, x, w: (y + k, z, c, x, w)))
    proj = jnp.concatenate(
        [p[:, :own_cols] for p in pieces] + [p[:, own_cols:] for p in pieces], axis=1
    )
    proj = (proj.astype(F32) + over_half(proj).astype(F32)).astype(BF)
    projs = [proj]
    for k in range(1, 4):
        projs.append(along_x(proj, k))

    hidden = emb.astype(F32) + proj.astype(F32)
    squares = jnp.broadcast_to(jnp.sum(hidden * hidden, axis=1, keepdims=True), (n, 128))
    total = squares
    for k in range(1, 4):
        total = total + route(squares, lambda y, z, c, x, w: (y, z + k, c, x, w))
    scale = lax.rsqrt(total / D + 1e-05)
    scales = [scale]
    for k in range(1, 4):
        scales.append(along_x(scale, k))

    packs = pack + [over_core(p) for p in pack]
    tick_c = (gain[:32] * 5.0 + 1.0).reshape(1, 32)
    base = based(embs, packs, tick_c)

    tick_a = (lengths.astype(F32) * 2.0 + 1.0).reshape(1, rows)
    pieces = list(verified_pieces(embs, projs, tick_a))
    for k in range(1, 4):
        pieces[k] = route(pieces[k], lambda y, z, c, x, w: (y - k, z, c, x, w))

    draft = drafted(embs, projs, scales, packs, base)
    total = draft[0].astype(F32)
    for k in range(1, 4):
        total = total + route(draft[k], lambda y, z, c, x, w: (y, z + k, c, x, w)).astype(F32)
    draft = total.astype(BF).reshape(rows, 2, steps, w_feat.shape[1])

    tick_b = (accepted.astype(F32) * 3.0 + 1.0).reshape(1, rows)
    other = over_core(second_halves(pieces, tick_b))
    verified = placed(pieces, other)
    return (verified.reshape(-1, own_cols), draft)


def solution(mesh):
    placed_in = (
        P("batch", None, None),
        P("batch"),
        P("batch"),
        P("batch", None, None, "heads"),
        P("batch", None, None, None, "heads"),
        P("batch", None, None, "heads"),
        P("heads", "batch"),
        P("heads", "batch"),
        P("batch"),
        P("batch", "heads"),
        P("batch", "heads"),
    )
    return jax.shard_map(
        step,
        mesh=mesh,
        in_specs=placed_in,
        out_specs=(P(None, "batch"), P("batch", None, None, "heads")),
        check_vma=False,
    )
```

```python
import jax
import jax.numpy as jnp
from jax import lax
from jax.experimental import pallas as pl
from jax.experimental.pallas import tpu as pltpu
from jax.sharding import PartitionSpec as P


D = 8192
HD = 128
Y, Z, C, X, W = 4, 4, 2, 4, 2
BF = jnp.bfloat16
F32 = jnp.float32


def route(array, move):
    pairs = []
    for y in range(Y):
        for z in range(Z):
            for c in range(C):
                for x in range(X):
                    for w in range(W):
                        ty, tz, tc, tx, tw = move(y, z, c, x, w)
                        ty, tz, tc, tx, tw = ty % Y, tz % Z, tc % C, tx % X, tw % W
                        source = ((y * Z + z) * C + c) * X * W + x * W + w
                        target = ((ty * Z + tz) * C + tc) * X * W + tx * W + tw
                        pairs.append((source, target))
    return lax.ppermute(array, ("batch", "heads"), pairs)


def among_y(array):
    groups = [[(y * Z + z) * C + c for y in range(Y)] for z in range(Z) for c in range(C)]
    return lax.all_to_all(array, "batch", 0, 0, axis_index_groups=groups, tiled=True)


def over_core(array):
    return route(array, lambda y, z, c, x, w: (y, z, c + 1, x, w))


def over_half(array):
    return route(array, lambda y, z, c, x, w: (y, z, c, x, w + 1))


def along_x(array, k):
    return route(array, lambda y, z, c, x, w: (y, z, c, x + k, w))


def from_everyone(array, axis):
    devices = lax.axis_size(axis)
    return lax.all_to_all(
        jnp.broadcast_to(array[None], (devices, *array.shape)), axis, 0, 0, tiled=True
    )


def risen(array, axis, start):
    n = array.shape[axis]
    twice = jnp.concatenate([array, array], axis=axis)
    return lax.dynamic_slice_in_dim(twice, start % n, n, axis)


def attend_local(queries, new_kv, cache_kv, lengths, accepted):
    rows, _, steps, qcols = queries.shape
    slots = cache_kv.shape[2]
    kv_heads = cache_kv.shape[3] // HD
    q_heads = qcols // HD
    group = q_heads // kv_heads
    qv = queries.reshape(rows, 2, steps, kv_heads, group, HD)
    keys = jnp.concatenate(
        [
            cache_kv[:, 0].reshape(rows, slots, kv_heads, HD),
            new_kv[:, :, 0].reshape(rows, 2 * steps, kv_heads, HD),
        ],
        axis=1,
    )
    vals = jnp.concatenate(
        [
            cache_kv[:, 1].reshape(rows, slots, kv_heads, HD),
            new_kv[:, :, 1].reshape(rows, 2 * steps, kv_heads, HD),
        ],
        axis=1,
    )
    scores = jnp.einsum(
        "rtigjd,rkgd->rtigjk", qv, keys, preferred_element_type=F32
    ) / jnp.sqrt(jnp.float32(HD))
    width = slots + 2 * steps
    slot = jnp.arange(width, dtype=jnp.int32)[None, None, None, :]
    rnd = jnp.arange(2, dtype=jnp.int32)[None, :, None, None]
    pos = jnp.arange(steps, dtype=jnp.int32)[None, None, :, None]
    first = slot - slots
    second = slot - slots - steps
    seen = slot < lengths[:, None, None, None]
    seen = seen | (first >= 0) & (first < steps) & (
        (rnd == 0) & (first <= pos) | (rnd == 1) & (first <= accepted[:, None, None, None])
    )
    seen = seen | (second >= 0) & (rnd == 1) & (second <= pos)
    seen = seen[:, :, :, None, None, :]
    masked = jnp.where(seen, scores, jnp.float32(-1e30))
    top = jnp.max(masked, axis=-1, keepdims=True)
    expo = jnp.where(seen, jnp.exp(masked - top), jnp.float32(0.0))
    weights = (expo / jnp.sum(expo, axis=-1, keepdims=True)).astype(BF)
    out = jnp.einsum("rtigjk,rkgd->rtigjd", weights, vals, preferred_element_type=F32)
    return out.astype(BF).reshape(rows * 2 * steps, qcols)


def position():
    b, h = lax.axis_index("batch"), lax.axis_index("heads")
    return b // (Z * C), b // C % Z, b % C, h // W


def joined_kernel(*refs):
    *ins, out_ref = refs
    width = ins[0].shape[1]
    for k, ref in enumerate(ins):
        out_ref[:, k * width : (k + 1) * width] = ref[...]


def joined(pieces):
    rows, width = pieces[0].shape
    return pl.pallas_call(
        joined_kernel, out_shape=jax.ShapeDtypeStruct((rows, width * len(pieces)), pieces[0].dtype)
    )(*pieces)


def regrouped_kernel(in_ref, out_ref):
    y = position()[0]
    width = in_ref.shape[2] // 2
    for k in range(4):
        for s in range(2):
            at = s * 4 + k
            out_ref[:, at * width : (at + 1) * width] = in_ref[
                (y + 4 - k) % 4, :, s * width : (s + 1) * width
            ]


def regrouped(array):
    _, rows, width = array.shape
    return pl.pallas_call(
        regrouped_kernel,
        out_shape=jax.ShapeDtypeStruct((rows, width * 4), array.dtype),
        name="regrouped",
    )(array)


def parted_kernel(in_ref, keep_ref, give_ref):
    y = position()[0]
    width = in_ref.shape[3]
    for k in range(4):
        keep_ref[:, k * width : (k + 1) * width] = in_ref[(y + 4 - k) % 4, 0]
        give_ref[:, k * width : (k + 1) * width] = in_ref[(y + 4 - k) % 4, 1]


def parted(array):
    _, _, rows, width = array.shape
    return pl.pallas_call(
        parted_kernel,
        out_shape=[jax.ShapeDtypeStruct((rows, width * 4), array.dtype)] * 2,
        name="parted",
    )(array)


def project_kernel(*refs):
    lines, own, other, out_ref = refs[:4], refs[4], refs[5], refs[7]
    attn, weights, sems = refs[8:]
    y, z, _, x = position()
    rows, (depth, cols) = lines[0].shape[0], own.shape[1:]
    copies = []
    for k in range(4):
        at = (k + z - x + 4) % 4
        copies.append(
            pltpu.make_async_copy(own.at[k], weights.at[at, :, pl.ds(0, cols)], sems.at[0, k])
        )
        copies.append(
            pltpu.make_async_copy(other.at[k], weights.at[at, :, pl.ds(cols, cols)], sems.at[1, k])
        )
        copies.append(
            pltpu.make_async_copy(lines[k], attn.at[pl.ds(k * rows, rows)], sems.at[2, k])
        )
    for copy in copies:
        copy.start()
    for copy in copies:
        copy.wait()
    total = None
    for k in range(4):
        part = jnp.dot(
            attn[:, k * depth : (k + 1) * depth], weights[k], preferred_element_type=F32
        )
        total = part if total is None else total + part
    total = total.astype(BF)
    for k in range(4):
        out_ref[(y + 4 - k) % 4] = total[k * rows : (k + 1) * rows]


def project(lines, own, other, after):
    rows, (depth, cols) = lines[0].shape[0], own.shape[1:]
    anywhere = pl.BlockSpec(memory_space=pl.ANY)
    return pl.pallas_call(
        project_kernel,
        in_specs=[anywhere] * 7,
        out_shape=jax.ShapeDtypeStruct((4, rows, 2 * cols), BF),
        scratch_shapes=[
            pltpu.VMEM((4 * rows, 4 * depth), BF),
            pltpu.VMEM((4, depth, 2 * cols), BF),
            pltpu.SemaphoreType.DMA((3, 4)),
        ],
        name="project",
    )(*lines, own, other, after)


def verified_kernel(*refs):
    embs, projs, outs = refs[:4], refs[4:8], refs[9:]
    rows, width = embs[0].shape
    cols = width // 8

    @pl.loop(0, rows // 16)
    def _(i):
        at = pl.multiple_of(i * 16, 16)
        for k in range(4):
            for e in range(4):
                for s in range(2):
                    cut = pl.ds((4 * s + e) * cols, cols)
                    hidden = embs[k][pl.ds(at, 16), cut].astype(F32)
                    hidden = hidden + projs[k][pl.ds(at, 16), cut].astype(F32)
                    outs[e][pl.ds(k * rows + at, 16), pl.ds(s * cols, cols)] = hidden.astype(BF)


def verified_pieces(embs, projs, after):
    rows, width = embs[0].shape
    return pl.pallas_call(
        verified_kernel,
        out_shape=[jax.ShapeDtypeStruct((4 * rows, width // 4), BF)] * 4,
        name="verified_pieces",
    )(*embs, *projs, after)


def based_kernel(*refs):
    embs, packs, out_ref, emb = refs[:4], refs[4:6], refs[7], refs[8]
    rows, width = embs[0].shape
    depth, tile = width // 8, 256
    for k in range(4):
        emb[k * rows : (k + 1) * rows] = embs[k][...]

    @pl.loop(0, out_ref.shape[1] // tile)
    def _(j):
        out = pl.ds(pl.multiple_of(j * tile, tile), tile)
        total = None
        for p in range(8):
            part = jnp.dot(
                emb[:, p * depth : (p + 1) * depth],
                packs[p // 4][p % 4, pl.ds(depth, depth), out],
                preferred_element_type=F32,
            )
            total = part if total is None else total + part
        out_ref[:, out] = total


def based(embs, packs, after):
    rows, width = embs[0].shape
    return pl.pallas_call(
        based_kernel,
        out_shape=jax.ShapeDtypeStruct((4 * rows, packs[0].shape[2]), F32),
        scratch_shapes=[pltpu.VMEM((4 * rows, width), BF)],
        name="based",
    )(*embs, *packs, after)


def draft_kernel(*refs):
    embs, projs, scales, packs, base_ref = refs[:4], refs[4:8], refs[8:12], refs[12:14], refs[14]
    outs, feat, sums = refs[15:19], refs[19], refs[20]
    _, z, _, x = position()
    rows, width = embs[0].shape
    depth, tile = width // 8, 256
    gains = []
    for p in range(8):
        extra = packs[p // 4][p % 4, 2 * depth : 2 * depth + 8, :depth].astype(F32)
        gains.append((extra[0:1] + extra[1:2]) + extra[2:3])
    for k in range(4):
        scale = scales[k][:, :1]
        for p in range(8):
            cut = slice(p * depth, (p + 1) * depth)
            hidden = embs[k][:, cut].astype(F32) + projs[k][:, cut].astype(F32)
            feat[k * rows : (k + 1) * rows, cut] = (hidden * scale * gains[p]).astype(BF)

    @pl.loop(0, outs[0].shape[1] // tile)
    def _(j):
        out = pl.ds(pl.multiple_of(j * tile, tile), tile)
        total = base_ref[:, out]
        for p in range(8):
            total = total + jnp.dot(
                feat[:, p * depth : (p + 1) * depth],
                packs[p // 4][p % 4, pl.ds(0, depth), out],
                preferred_element_type=F32,
            )
        sums[:, :, out] = total.astype(BF).reshape(4, rows, tile)

    for k in range(4):
        outs[k][...] = sums[(x - z - k + 8) % 4]


def drafted(embs, projs, scales, packs, base):
    rows, width = embs[0].shape
    cols = packs[0].shape[2]
    return pl.pallas_call(
        draft_kernel,
        out_shape=[jax.ShapeDtypeStruct((rows, cols), BF)] * 4,
        scratch_shapes=[
            pltpu.VMEM((4 * rows, width), BF),
            pltpu.VMEM((4, rows, cols), BF),
        ],
        name="drafted",
    )(*embs, *projs, *scales, *packs, base)


def halves_kernel(*refs):
    ins, out_ref = refs[:4], refs[-1]
    cols = out_ref.shape[2]
    for k, ref in enumerate(ins):
        out_ref[k] = ref[:, cols:]


def second_halves(pieces, after):
    rows, width = pieces[0].shape
    return pl.pallas_call(
        halves_kernel,
        out_shape=jax.ShapeDtypeStruct((4, rows, width // 2), BF),
        name="second_halves",
    )(*pieces, after)


def placed_kernel(*refs):
    pieces, other_ref, out_ref = refs[:4], refs[4], refs[5]
    y, _, c, x = position()
    rows, cols = out_ref.shape[2:]
    for e in range(4):
        for k in range(4):
            at = (y + e) % 4 * 4 + (x + 4 - k) % 4
            cut = slice(k * rows, (k + 1) * rows)
            out_ref[at, c] = pieces[e][cut, :cols]
            out_ref[at, 1 - c] = other_ref[e, cut]


def placed(pieces, other):
    rows, width = pieces[0].shape
    return pl.pallas_call(
        placed_kernel,
        out_shape=jax.ShapeDtypeStruct((16, 2, rows // 4, width // 2), BF),
        name="placed",
    )(*pieces, other)


def step(
    token_ids, accepted, lengths, queries, new_kv, cache_kv, table, w_out, gain, w_feat, w_emb
):
    rows, _, steps = token_ids.shape
    n = rows * 2 * steps
    _, _, c, x = position()
    h = lax.axis_index("heads")
    own_cols = w_out.shape[1]

    outs = [w_out]
    for k in range(1, 4):
        outs.append(route(w_out, lambda y, z, c, x, w: (y, z, c, x + k, w)))

    ids = from_everyone(token_ids.reshape(-1), "batch").reshape(Y, Z, C, n)
    ids = risen(risen(ids, 1, x), 2, c)
    ids = jnp.swapaxes(ids, 0, 1).reshape(-1)

    high = gain.astype(BF)
    mid = (gain - high.astype(F32)).astype(BF)
    low = (gain - high.astype(F32) - mid.astype(F32)).astype(BF)
    extra = jnp.stack([high, mid, low])
    extra = jnp.pad(extra, ((0, 13), (0, w_feat.shape[1] - extra.shape[1])))
    pack = [jnp.concatenate([w_feat, w_emb, extra], axis=0)]
    for k in range(1, 4):
        pack.append(route(pack[0], lambda y, z, c, x, w: (y + k, z, c, x, w)))

    attn = attend_local(queries, new_kv, cache_kv, lengths, accepted)
    slots = []
    for k in range(4):
        slots.append(route(attn, lambda y, z, c, x, w: (y, x + k, c, z, w)))
    attn = joined(slots)
    lines = [attn]
    for k in range(1, 4):
        lines.append(route(attn, lambda y, z, c, x, w: (y + k, z, c, x, w)))

    vocab_rows = table.shape[0]
    local_ids = ids - h * vocab_rows
    inside = ((local_ids >= 0) & (local_ids < vocab_rows)).reshape(-1, 128)
    local_ids = jnp.clip(local_ids, 0, vocab_rows - 1)
    eye = jnp.arange(128)[:, None] == jnp.arange(128)[None, :]
    found = table.at[local_ids].get(mode="promise_in_bounds")
    keep = (eye[None] & inside[:, None, :]).astype(BF)
    found = lax.dot_general(
        keep,
        found.reshape(-1, 128, own_cols),
        (((2,), (1,)), ((0,), (0,))),
        preferred_element_type=F32,
    )
    found = found.astype(BF).reshape(4, 4 * 2 * n, own_cols)
    emb = found[0]
    for k in (2, 1, 3):
        emb = emb + along_x(found[k], k)
    emb = emb.reshape(4, 2, n, own_cols)
    emb = among_y(emb)
    keep, give = parted(emb)
    got = over_core(give)
    emb = jnp.concatenate([keep, got], axis=1)
    emb = lax.optimization_barrier(emb + over_half(emb))
    embs = [emb]
    for k in range(1, 4):
        embs.append(along_x(emb, k))

    tick_d = (gain[:32] * 5.0 + 1.0).reshape(1, 32)
    outs = jnp.stack(outs)
    part = project(lines, outs, over_core(outs), tick_d)
    part = among_y(part)
    proj = regrouped(part)
    proj = (proj.astype(F32) + over_half(proj).astype(F32)).astype(BF)
    proj = lax.optimization_barrier(proj)
    projs = [proj]
    for k in range(1, 4):
        projs.append(along_x(proj, k))

    hidden = emb.astype(F32) + proj.astype(F32)
    squares = jnp.broadcast_to(jnp.sum(hidden * hidden, axis=1, keepdims=True), (n, 128))
    total = squares + route(squares, lambda y, z, c, x, w: (y, z ^ 1, c, x, w))
    total = total + route(total, lambda y, z, c, x, w: (y, z ^ 2, c, x, w))
    scale = lax.rsqrt(total / D + 1e-05)
    scales = [scale]
    for k in range(1, 4):
        scales.append(along_x(scale, k))

    packs = jnp.stack(pack)
    packs = [packs, over_core(packs)]
    tick_e = (token_ids[:, 0, 0].astype(F32) * 7.0 + 1.0).reshape(1, rows)
    base = based(embs, packs, tick_e)

    tick_a = (lengths.astype(F32) * 2.0 + 1.0).reshape(1, rows)
    pieces = list(verified_pieces(embs, projs, tick_a))
    for k in range(1, 4):
        pieces[k] = route(pieces[k], lambda y, z, c, x, w: (y - k, z, c, x, w))

    draft = drafted(embs, projs, scales, packs, base)
    total = draft[0].astype(F32)
    for k in range(1, 4):
        total = total + route(draft[k], lambda y, z, c, x, w: (y, z + k, c, x, w)).astype(F32)
    draft = total.astype(BF).reshape(rows, 2, steps, w_feat.shape[1])

    tick_b = (accepted.astype(F32) * 3.0 + 1.0).reshape(1, rows)
    other = over_core(second_halves(pieces, tick_b))
    verified = placed(pieces, other)
    return (verified.reshape(-1, own_cols), draft)


def solution(mesh):
    placed_in = (
        P("batch", None, None),
        P("batch"),
        P("batch"),
        P("batch", None, None, "heads"),
        P("batch", None, None, None, "heads"),
        P("batch", None, None, "heads"),
        P("heads", "batch"),
        P("heads", "batch"),
        P("batch"),
        P("batch", "heads"),
        P("batch", "heads"),
    )
    return jax.shard_map(
        step,
        mesh=mesh,
        in_specs=placed_in,
        out_specs=(P(None, "batch"), P("batch", None, None, "heads")),
        check_vma=False,
    )
```
